32 devices in a mesh: layer: 2 (over x), lat: 16 (over z, y, core).
Axes of the slice: x: 2, y: 2, z: 4, core: 2. Of those that a mesh axis runs over, the one named last changes fastest.
Arguments:
- acts: bfloat16 [2, 256, 1280], P('layer', 'lat'), may hold values from -6 to 6
- enc_weight: bfloat16 [2, 1280, 8192], P('layer', None, 'lat'), may hold values from -0.15625 to 0.15625
- enc_bias: float32 [2, 8192], P('layer', 'lat'), may hold values from -3 to 3
- dec_weight: bfloat16 [2, 2, 8192, 1280], P('layer', None, 'lat'), may hold values from -0.0625 to 0.0625
- dec_bias: float32 [2, 1280], P('layer'), may hold values from -3 to 3
Outputs:
- recon: bfloat16 [2, 256, 1280], P('layer', 'lat')
The draws below stay inside these ranges and needn't reach their ends.
All inputs are finite; a program needn't handle non-finite values.
Results may differ from the reference program's by a relative error of at most 0.0048.
Values may be sent and summed in bfloat16 or wider, within the bound.
No kernel may reach another device: no remote copies, remote signals or barrier semaphores. Data moves between devices by JAX's collectives and lax.ppermute only.
A program may use at most 128 MiB of HBM per device.

```python
import jax
import jax.numpy as jnp

D = 1280
LATENTS = 8192
TOKENS = 256
LAYERS = 2


def levels(key, shape, cuts, low, largest):
    factor_of = 1.0
    for position, blocks in cuts:
        steps = jax.random.uniform(jax.random.fold_in(jax.random.fold_in(key, 6), position), (blocks,), jnp.float32, low / len(cuts), largest / len(cuts))
        factor_of = factor_of * jnp.repeat(jnp.exp(steps), shape[position] // blocks).reshape((-1,) + (1,) * (len(shape) - 1 - position))
    return factor_of


def normal_values(stream_key, extent, spread, limit, cuts=(), held_as=jnp.bfloat16):
    factor_of = levels(stream_key, extent, cuts, -0.22, 0.18) if cuts else 1.0
    result = jax.random.normal(stream_key, extent, jnp.float32) * spread * factor_of
    return jnp.minimum(jnp.maximum(result, -limit), limit).astype(held_as)


def setup_inputs(seed: int = 0) -> dict:
    splits = jax.random.split(jax.random.key(seed), 6)
    acts = normal_values(splits[0], (LAYERS, TOKENS, D), 1.0, 6.0, ((0, 2), (1, 16)))
    enc_weight = normal_values(splits[1], (LAYERS, D, LATENTS), D ** -0.5, 0.15625, ((0, 2), (2, 16)))
    enc_bias = normal_values(splits[2], (LAYERS, LATENTS), 0.5, 3.0, ((0, 2), (1, 16)), jnp.float32)
    dec_weight = normal_values(splits[3], (LAYERS, LAYERS, LATENTS, D), LATENTS ** -0.5, 0.0625, ((0, 2), (2, 16)))
    dec_bias = normal_values(splits[4], (LAYERS, D), 0.5, 3.0, ((0, 2),), jnp.float32)
    return {"acts": acts, "enc_weight": enc_weight, "enc_bias": enc_bias, "dec_weight": dec_weight, "dec_bias": dec_bias}


def reference(acts, enc_weight, enc_bias, dec_weight, dec_bias):
    latents = []
    for source in range(LAYERS):
        pre = jnp.dot(acts[source], enc_weight[source], preferred_element_type=jnp.float32) + enc_bias[source]
        latents.append(jnp.maximum(pre, 0.0).astype(jnp.bfloat16))
    results = []
    for target in range(LAYERS):
        total = jnp.zeros((TOKENS, D), jnp.float32)
        for source in range(target + 1):
            total = total + jnp.dot(latents[source], dec_weight[source, target], preferred_element_type=jnp.float32)
        results.append((total + dec_bias[target][None, :]).astype(jnp.bfloat16))
    return jnp.stack(results, axis=0)
```

```python
import jax
import jax.numpy as jnp
from jax import lax
from jax.sharding import PartitionSpec as P


BF16 = jnp.bfloat16
F32 = jnp.float32


def factors(n):
    core = min(2, n)
    outer = min(4, n // core)
    return outer, n // core // outer, core


def swap(x, n, k):
    return lax.ppermute(x, "lat", [(i, i ^ k) for i in range(n)])


def local(acts, enc_weight, enc_bias, dec_weight, dec_bias):
    layers = lax.axis_size("layer")
    n = lax.axis_size("lat")
    source = lax.axis_index("layer")
    outer, middle, core = factors(n)
    rows, width = acts.shape[1:]

    x = acts[0]
    x = jnp.concatenate([x] + [swap(x, n, k * middle * core) for k in range(1, outer)], 0)
    x = jnp.concatenate([x] + [swap(x, n, k * core) for k in range(1, middle)], 0)
    x = jnp.concatenate([x] + [swap(x, n, k) for k in range(1, core)], 0)

    pre = jnp.dot(x, enc_weight[0], preferred_element_type=F32) + enc_bias[0][None, :]
    latent = jnp.maximum(pre, 0.0).astype(BF16)

    def reduce(part, count, unit):
        pieces = part.reshape(count, -1, width)
        got = [swap(pieces[k].astype(BF16), n, k * unit) for k in range(1, count)]
        total = pieces[0]
        for piece in got:
            total = total + piece.astype(F32)
        return total

    total = None
    for d in reversed(range(layers)):
        target = jnp.minimum(source + d, layers - 1)
        matrix = lax.dynamic_index_in_dim(dec_weight[0], target, 0, keepdims=False)
        part = jnp.dot(latent, matrix, preferred_element_type=F32)
        part = reduce(part, core, 1)
        part = reduce(part, middle, core)
        part = reduce(part, outer, middle * core)
        if d:
            pairs = [(i, i + d) for i in range(layers - d)]
            part = lax.ppermute(part.astype(BF16), "layer", pairs).astype(F32)
        total = part if total is None else total + part
    return (total + dec_bias[0][None, :]).astype(BF16)[None]


def solution(mesh):
    return jax.shard_map(
        local,
        mesh=mesh,
        in_specs=(
            P("layer", "lat", None),
            P("layer", None, "lat"),
            P("layer", "lat"),
            P("layer", None, "lat", None),
            P("layer", None),
        ),
        out_specs=P("layer", "lat", None),
        check_vma=False,
    )
```

```python
import functools

import jax
import jax.numpy as jnp
from jax import lax
from jax.experimental import pallas as pl
from jax.experimental.pallas import tpu as pltpu
from jax.sharding import PartitionSpec as P


BF16 = jnp.bfloat16
F32 = jnp.float32
VMEM = pl.BlockSpec(memory_space=pltpu.VMEM)
HBM = pl.BlockSpec(memory_space=pltpu.HBM)
SMEM = pl.BlockSpec(memory_space=pltpu.SMEM)
MIB = 1 << 20


def factors(n):
    core = min(2, n)
    outer = min(4, n // core)
    return outer, n // core // outer, core


def swap(x, n, k):
    return lax.ppermute(x, "lat", [(i, i ^ k) for i in range(n)])


def stack_kernel(*refs):
    out = refs[-1]
    at = 0
    for ref in refs[:-1]:
        out[pl.ds(at, ref.shape[0]), :] = ref[...]
        at += ref.shape[0]


def stack(pieces):
    if len(pieces) == 1:
        return pieces[0]
    rows = sum(p.shape[0] for p in pieces)
    return pl.pallas_call(
        stack_kernel,
        out_shape=jax.ShapeDtypeStruct((rows, pieces[0].shape[1]), pieces[0].dtype),
        in_specs=[VMEM] * len(pieces),
        out_specs=VMEM,
        compiler_params=pltpu.CompilerParams(vmem_limit_bytes=4 * MIB),
        cost_estimate=pl.CostEstimate(flops=1000000, bytes_accessed=rows * 5120, transcendentals=0),
    )(*pieces)


def load_kernel(count, *refs):
    sems = refs[2 * count]
    copies = [pltpu.make_async_copy(refs[i], refs[count + i], sems.at[i]) for i in range(count)]
    for copy in copies:
        copy.start()
    for copy in copies:
        copy.wait()


def load(*arrays):
    arrays = [pltpu.with_memory_space_constraint(a, pltpu.HBM) for a in arrays]
    return pl.pallas_call(
        functools.partial(load_kernel, len(arrays)),
        out_shape=[jax.ShapeDtypeStruct(a.shape, a.dtype) for a in arrays],
        in_specs=[HBM] * len(arrays),
        out_specs=[VMEM] * len(arrays),
        scratch_shapes=[pltpu.SemaphoreType.DMA((len(arrays),))],
        compiler_params=pltpu.CompilerParams(vmem_limit_bytes=8 * MIB),
        cost_estimate=pl.CostEstimate(flops=1000000, bytes_accessed=4 * MIB, transcendentals=0),
        name="load",
    )(*arrays)


def encode_kernel(xs, core, x_refs, w_refs, b_refs, latent, x_all):
    at = 0
    for ref in x_refs:
        x_all[pl.ds(at, ref.shape[0]), :] = ref[...]
        at += ref.shape[0]
    for c in range(core):
        size = w_refs[c].shape[2]
        pre = jnp.dot(x_all[...], w_refs[c][0], preferred_element_type=F32) + b_refs[c][...]
        latent[:, c * size : (c + 1) * size] = jnp.maximum(pre, 0.0).astype(BF16)


def decode_part(target, latent, w_refs):
    total = None
    for c, w in enumerate(w_refs):
        size = w.shape[2]
        part = jnp.dot(latent[:, c * size : (c + 1) * size], w[0, target], preferred_element_type=F32)
        total = part if total is None else total + part
    return total


def first_kernel(xs, core, middle, d, layers, *refs):
    x_refs, refs = refs[:xs], refs[xs:]
    w_refs, refs = refs[:core], refs[core:]
    b_refs, refs = refs[:core], refs[core:]
    d_refs, refs = refs[:core], refs[core:]
    latent, outs, x_all = refs[0], refs[1:-1], refs[-1]
    encode_kernel(xs, core, x_refs, w_refs, b_refs, latent, x_all)
    decode_store(core, middle, d, layers, latent, d_refs, outs)


def next_kernel(core, middle, d, layers, latent, *refs):
    decode_store(core, middle, d, layers, latent, refs[:core], refs[core:])


def decode_store(core, middle, d, layers, latent, d_refs, outs):
    target = lax.axis_index("layer") + d

    @pl.when(target < layers)
    def _():
        total = decode_part(target, latent, d_refs)
        rows = total.shape[0] // middle
        for k in range(middle):
            outs[k][...] = total[k * rows : (k + 1) * rows].astype(outs[k].dtype)

    @pl.when(target >= layers)
    def _():
        for out in outs:
            out[...] = jnp.zeros_like(out)


def local(acts, enc_weight, enc_bias, dec_weight, dec_bias):
    layers = lax.axis_size("layer")
    n = lax.axis_size("lat")
    outer, middle, core = factors(n)
    width = acts.shape[2]
    size = enc_weight.shape[2]

    own = acts[0]
    pieces = [swap(own, n, k * middle * core) for k in range(1, outer)]
    own, enc, bias, dec = load(own, enc_weight, enc_bias, dec_weight)
    pieces = [own] + pieces
    enc = [enc] + [swap(enc_weight, n, k) for k in range(1, core)]
    bias = [bias] + [swap(enc_bias, n, k) for k in range(1, core)]
    dec = [dec] + [swap(dec_weight, n, k) for k in range(1, core)]
    column = stack(pieces)
    xs = [column] + [swap(column, n, k * core) for k in range(1, middle)]
    rows = column.shape[0]

    def outs(d):
        return [jax.ShapeDtypeStruct((rows, width), F32 if d == 0 and k == 0 else BF16) for k in range(middle)]

    flops = 2 * rows * middle * core * size * width
    latent = None
    received = []
    for d in reversed(range(layers)):
        if latent is None:
            latent, *parts = pl.pallas_call(
                functools.partial(first_kernel, len(xs), core, middle, d, layers),
                out_shape=[jax.ShapeDtypeStruct((rows * middle, core * size), BF16)] + outs(d),
                in_specs=[VMEM] * (len(xs) + 3 * core),
                out_specs=[VMEM] * (1 + middle),
                scratch_shapes=[pltpu.VMEM((rows * middle, width), BF16)],
                compiler_params=pltpu.CompilerParams(vmem_limit_bytes=8 * MIB),
                cost_estimate=pl.CostEstimate(flops=2 * flops, bytes_accessed=8 * MIB, transcendentals=0),
            )(*xs, *enc, *bias, *dec)
        else:
            parts = pl.pallas_call(
                functools.partial(next_kernel, core, middle, d, layers),
                out_shape=outs(d),
                in_specs=[VMEM] * (1 + core),
                out_specs=[VMEM] * middle,
                compiler_params=pltpu.CompilerParams(vmem_limit_bytes=8 * MIB),
                cost_estimate=pl.CostEstimate(flops=flops, bytes_accessed=4 * MIB, transcendentals=0),
            )(latent, *dec)
        for k in range(middle):
            if d or k:
                pairs = [
                    (l * n + i, (l + d) % layers * n + (i ^ (k * core)))
                    for l in range(layers)
                    for i in range(n)
                ]
                received.append(lax.ppermute(parts[k], ("layer", "lat"), pairs))
            else:
                total = parts[0]
    for piece in received:
        total = total + piece.astype(F32)
    pieces = total.reshape(outer, -1, width)
    total = pieces[0]
    for k in range(1, outer):
        total = total + swap(pieces[k].astype(BF16), n, k * middle * core).astype(F32)
    return (total + dec_bias[0][None, :]).astype(BF16)[None]


def solution(mesh):
    return jax.shard_map(
        local,
        mesh=mesh,
        in_specs=(
            P("layer", "lat", None),
            P("layer", None, "lat"),
            P("layer", "lat"),
            P("layer", None, "lat", None),
            P("layer", None),
        ),
        out_specs=P("layer", "lat", None),
        check_vma=False,
    )
```

```python
import functools

import jax
import jax.numpy as jnp
from jax import lax
from jax.experimental import pallas as pl
from jax.experimental.pallas import tpu as pltpu
from jax.sharding import PartitionSpec as P


BF16 = jnp.bfloat16
F32 = jnp.float32
VMEM = pl.BlockSpec(memory_space=pltpu.VMEM)
HBM = pl.BlockSpec(memory_space=pltpu.HBM)
MIB = 1 << 20


def factors(n):
    core = min(2, n)
    outer = min(4, n // core)
    return outer, n // core // outer, core


def swap(x, n, k):
    return lax.ppermute(x, "lat", [(i, i ^ k) for i in range(n)])


def call(kernel, outs, args, specs=None, scratch=(), flops=1000000):
    return pl.pallas_call(
        kernel,
        out_shape=outs,
        in_specs=specs or [VMEM] * len(args),
        out_specs=[VMEM] * len(outs),
        scratch_shapes=list(scratch),
        compiler_params=pltpu.CompilerParams(vmem_limit_bytes=8 * MIB),
        cost_estimate=pl.CostEstimate(flops=flops, bytes_accessed=MIB, transcendentals=0),
    )(*args)


def load_kernel(count, *refs):
    sems = refs[2 * count]
    copies = [pltpu.make_async_copy(refs[i], refs[count + i], sems.at[i]) for i in range(count)]
    for copy in copies:
        copy.start()
    for copy in copies:
        copy.wait()


def load(*arrays):
    arrays = [pltpu.with_memory_space_constraint(a, pltpu.HBM) for a in arrays]
    count = len(arrays)
    return call(
        functools.partial(load_kernel, count),
        [jax.ShapeDtypeStruct(a.shape, a.dtype) for a in arrays],
        arrays,
        specs=[HBM] * count,
        scratch=[pltpu.SemaphoreType.DMA((count,))],
    )


def stack_kernel(*refs):
    out = refs[-1]
    at = 0
    for ref in refs[:-1]:
        out[pl.ds(at, ref.shape[0]), :] = ref[...]
        at += ref.shape[0]


def stack(pieces):
    rows = sum(p.shape[0] for p in pieces)
    shape = jax.ShapeDtypeStruct((rows, pieces[0].shape[1]), pieces[0].dtype)
    return call(stack_kernel, [shape], pieces)[0]


def encode(x, w_refs, b_refs, latent):
    for c, (w, b) in enumerate(zip(w_refs, b_refs)):
        size = w.shape[2]
        pre = jnp.dot(x[...], w[0], preferred_element_type=F32) + b[...]
        latent[:, c * size : (c + 1) * size] = jnp.maximum(pre, 0.0).astype(BF16)


def decode(latent, w_refs, d, layers, out):
    target = lax.axis_index("layer") + d

    @pl.when(target < layers)
    def _():
        total = None
        for c, w in enumerate(w_refs):
            size = w.shape[2]
            part = jnp.dot(latent[:, c * size : (c + 1) * size], w[0, target], preferred_element_type=F32)
            total = part if total is None else total + part
        out[...] = total.astype(out.dtype)

    if d:

        @pl.when(target >= layers)
        def _():
            out[...] = jnp.zeros_like(out)


def encode_kernel(core, ds, layers, x, *refs):
    w_refs, b_refs, d_refs = refs[:core], refs[core : 2 * core], refs[2 * core : 3 * core]
    latent, outs = refs[3 * core], refs[3 * core + 1 :]
    encode(x, w_refs, b_refs, latent)
    for d, out in zip(ds, outs):
        decode(latent, d_refs, d, layers, out)


def decode_kernel(core, layers, latent, *refs):
    decode(latent, refs[:core], 0, layers, refs[core])


def work(acts, enc_weight, enc_bias, dec_weight, dec_bias):
    layers = lax.axis_size("layer")
    n = lax.axis_size("lat")
    outer, middle, core = factors(n)
    width = acts.shape[2]
    size = enc_weight.shape[2]

    pieces = [swap(acts[0], n, k * middle * core) for k in range(1, outer)]
    enc = [swap(enc_weight, n, k) for k in range(1, core)]
    dec = [swap(dec_weight, n, k) for k in range(1, core)]
    bias = [swap(enc_bias, n, k) for k in range(1, core)]
    own, own_enc, own_bias, own_dec = load(acts[0], enc_weight, enc_bias, dec_weight)
    enc, dec, bias = [own_enc] + enc, [own_dec] + dec, [own_bias] + bias
    column = stack([own] + pieces)
    xs = [column] + [swap(column, n, k * core) for k in range(1, middle)]
    rows = column.shape[0]
    flops = 2 * rows * core * size * width
    hidden = jax.ShapeDtypeStruct((rows, core * size), BF16)

    def send(part, d, k):
        pairs = [
            (l * n + i, (l + d) % layers * n + (i ^ (k * core) if l + d < layers else i))
            for l in range(layers)
            for i in range(n)
        ]
        return lax.ppermute(part, ("layer", "lat"), pairs)

    received = []
    total = None
    later = list(range(layers - 1, 0, -1))
    for k, x in enumerate(xs):
        ds = later if k else later + [0]
        outs = [jax.ShapeDtypeStruct((rows, width), BF16 if d else F32) for d in ds]
        latent, *parts = call(
            functools.partial(encode_kernel, core, ds, layers),
            [hidden] + outs,
            [x] + enc + bias + dec,
            flops=flops * (1 + len(ds)),
        )
        for d, part in zip(ds, parts):
            if d:
                received.append(send(part, d, k))
            else:
                total = part
        if k:
            part = call(
                functools.partial(decode_kernel, core, layers),
                [jax.ShapeDtypeStruct((rows, width), BF16)],
                [latent] + dec,
                flops=flops,
            )[0]
            received.append(send(part, 0, k))
    for piece in received:
        total = total + piece.astype(F32)
    pieces = total.reshape(outer, -1, width)
    total = pieces[0]
    for k in range(1, outer):
        total = total + swap(pieces[k].astype(BF16), n, k * middle * core).astype(F32)
    return (total + dec_bias[0][None, :]).astype(BF16)[None]


def solution(mesh):
    return jax.shard_map(
        work,
        mesh=mesh,
        in_specs=(
            P("layer", "lat", None),
            P("layer", None, "lat"),
            P("layer", "lat"),
            P("layer", None, "lat", None),
            P("layer", None),
        ),
        out_specs=P("layer", "lat", None),
        check_vma=False,
    )
```

```python
import functools

import jax
import jax.numpy as jnp
from jax import lax
from jax.experimental import pallas as pl
from jax.experimental.pallas import tpu as pltpu
from jax.sharding import PartitionSpec as P


BF16 = jnp.bfloat16
F32 = jnp.float32
VMEM = pl.BlockSpec(memory_space=pltpu.VMEM)
HBM = pl.BlockSpec(memory_space=pltpu.HBM)
MIB = 1 << 20


def factors(n):
    core = min(2, n)
    outer = min(4, n // core)
    return outer, n // core // outer, core


def zstep(k, middle, core):
    return k * middle * core + core - 1


def swap(x, n, k):
    return lax.ppermute(x, "lat", [(i, i ^ k) for i in range(n)])


def call(kernel, outs, args, specs=None, scratch=(), flops=1000000):
    return pl.pallas_call(
        kernel,
        out_shape=outs,
        in_specs=specs or [VMEM] * len(args),
        out_specs=[VMEM] * len(outs),
        scratch_shapes=list(scratch),
        compiler_params=pltpu.CompilerParams(vmem_limit_bytes=8 * MIB),
        cost_estimate=pl.CostEstimate(flops=flops, bytes_accessed=MIB, transcendentals=0),
    )(*args)


def load_kernel(count, *refs):
    sems = refs[2 * count]
    copies = [pltpu.make_async_copy(refs[i], refs[count + i], sems.at[i]) for i in range(count)]
    for copy in copies:
        copy.start()
    for copy in copies:
        copy.wait()


def load(*arrays):
    arrays = [pltpu.with_memory_space_constraint(a, pltpu.HBM) for a in arrays]
    count = len(arrays)
    return call(
        functools.partial(load_kernel, count),
        [jax.ShapeDtypeStruct(a.shape, a.dtype) for a in arrays],
        arrays,
        specs=[HBM] * count,
        scratch=[pltpu.SemaphoreType.DMA((count,))],
    )


def stack_kernel(*refs):
    out = refs[-1]
    at = 0
    for ref in refs[:-1]:
        out[pl.ds(at, ref.shape[0]), :] = ref[...]
        at += ref.shape[0]


def stack(pieces):
    rows = sum(p.shape[0] for p in pieces)
    shape = jax.ShapeDtypeStruct((rows, pieces[0].shape[1]), pieces[0].dtype)
    return call(stack_kernel, [shape], pieces)[0]


def encode(x, w_refs, b_refs, latent):
    for c, (w, b) in enumerate(zip(w_refs, b_refs)):
        size = w.shape[2]
        pre = jnp.dot(x[...], w[0], preferred_element_type=F32) + b[...]
        latent[:, c * size : (c + 1) * size] = jnp.maximum(pre, 0.0).astype(BF16)


def decode(latent, w_refs, d, layers, outs):
    target = lax.axis_index("layer") + d

    @pl.when(target < layers)
    def _():
        total = None
        for c, w in enumerate(w_refs):
            size = w.shape[2]
            part = jnp.dot(latent[:, c * size : (c + 1) * size], w[0, target], preferred_element_type=F32)
            total = part if total is None else total + part
        at = 0
        for out in outs:
            out[...] = total[at : at + out.shape[0]].astype(out.dtype)
            at += out.shape[0]

    if d:

        @pl.when(target >= layers)
        def _():
            for out in outs:
                out[...] = jnp.zeros_like(out)


def encode_kernel(core, slots, plan, layers, *refs):
    xs = 1 + max(at[0] for at in slots)
    x_refs, refs = refs[:xs], refs[xs:]
    w_refs, b_refs, d_refs = refs[:core], refs[core : 2 * core], refs[2 * core : 3 * core]
    latent, outs, x = refs[3 * core], refs[3 * core + 1 : -1], refs[-1]
    at = 0
    for which, first, rows in slots:
        x[pl.ds(at, rows), :] = x_refs[which][pl.ds(first, rows), :]
        at += rows
    encode(x, w_refs, b_refs, latent)
    for d, groups in plan:
        decode(latent, d_refs, d, layers, outs[:groups])
        outs = outs[groups:]


def decode_kernel(core, layers, latent, *refs):
    decode(latent, refs[:core], 0, layers, refs[core:])


def sum_kernel(ats, block, *refs):
    parts, outs = refs[: len(ats)], refs[len(ats) :]
    for j, out in enumerate(outs):
        total = None
        for at, ref in zip(ats, parts):
            part = ref[pl.ds(at + j * block, block), :].astype(F32)
            total = part if total is None else total + part
        out[...] = total.astype(out.dtype)


def work(acts, enc_weight, enc_bias, dec_weight, dec_bias):
    layers = lax.axis_size("layer")
    n = lax.axis_size("lat")
    outer, middle, core = factors(n)
    width = acts.shape[2]
    size = enc_weight.shape[2]

    pieces = [swap(acts[0], n, zstep(k, middle, core)) for k in range(1, outer)]
    enc = [swap(enc_weight, n, k) for k in range(1, core)]
    dec = [swap(dec_weight, n, k) for k in range(1, core)]
    bias = [swap(enc_bias, n, k) for k in range(1, core)]
    own, own_enc, own_bias, own_dec = load(acts[0], enc_weight, enc_bias, dec_weight)
    enc, dec, bias = [own_enc] + enc, [own_dec] + dec, [own_bias] + bias
    block = own.shape[0]
    rows = block * outer
    flops = 2 * rows * core * size * width
    hidden = jax.ShapeDtypeStruct((rows, core * size), BF16)

    blocks = [own] + pieces
    batches = [[0] + list(range(outer - 1, 0, -1))[:1], list(range(1, outer - 1))]
    batches = [batch for batch in batches if batch]
    stacks = [stack([blocks[k] for k in batch]) for batch in batches]
    slots = [None] * outer
    for i, batch in enumerate(batches):
        for j, k in enumerate(batch):
            slots[k] = (i, j * block, block)
    xs = [(blocks, [(k, 0, block) for k in range(outer)])]
    for k in range(1, middle):
        xs.append(([swap(x, n, k * core) for x in stacks], slots))

    groups = cuts(outer)
    order = [k for group in groups for k in group]

    def send(part, d, k):
        pairs = [
            (l * n + i, (l + d) % layers * n + (i ^ (k * core) if l + d < layers else i))
            for l in range(layers)
            for i in range(n)
        ]
        return lax.ppermute(part, ("layer", "lat"), pairs)

    def shapes(dtype, whole=False):
        sizes = [rows] if whole else [block * len(group) for group in groups]
        return [jax.ShapeDtypeStruct((size, width), dtype) for size in sizes]

    totals = [[] for _ in groups]
    later = list(range(layers - 1, 0, -1))
    for k, (x, where) in enumerate(xs):
        plan = [(d, len(groups) if k else 1) for d in later] + ([] if k else [(0, len(groups))])
        outs = [shape for d, _ in plan for shape in shapes(BF16 if d else F32, d > 0 and k == 0)]
        latent, *parts = call(
            functools.partial(encode_kernel, core, [where[j] for j in order], plan, layers),
            [hidden] + outs,
            x + enc + bias + dec,
            scratch=[pltpu.VMEM((rows, width), BF16)],
            flops=flops * (1 + len(plan)),
        )
        if k == 0:
            for d in later:
                got = send(parts.pop(0), d, k)
                at = 0
                for total, group in zip(totals, groups):
                    total.append((at, got))
                    at += block * len(group)
            for total in totals:
                total.insert(0, (0, parts.pop(0)))
        else:
            own_parts = call(
                functools.partial(decode_kernel, core, layers),
                shapes(BF16),
                [latent] + dec,
                flops=flops,
            )
            for g, total in enumerate(totals):
                for i, d in enumerate(later):
                    total.append((0, send(parts[i * len(groups) + g], d, k)))
                total.append((0, send(own_parts[g], 0, k)))
    result = None
    near = []
    for total, group in zip(totals, groups):
        pieces = call(
            functools.partial(sum_kernel, [at for at, _ in total], block),
            [jax.ShapeDtypeStruct((block, width), BF16 if k else F32) for k in group],
            [part for _, part in total],
        )
        for k, piece in zip(group, pieces):
            if k:
                near.append(swap(piece, n, zstep(k, middle, core)))
            else:
                result = piece
    for piece in near:
        result = result + piece.astype(F32)
    return (result + dec_bias[0][None, :]).astype(BF16)[None]


def cuts(outer):
    far = list(range(outer - 1, 0, -1))
    half = len(far) - max(outer // 2 - 1, 0)
    return [group for group in (far[:half], far[half:] + [0]) if group]


def solution(mesh):
    return jax.shard_map(
        work,
        mesh=mesh,
        in_specs=(
            P("layer", "lat", None),
            P("layer", None, "lat"),
            P("layer", "lat"),
            P("layer", None, "lat", None),
            P("layer", None),
        ),
        out_specs=P("layer", "lat", None),
        check_vma=False,
    )
```

```python
import functools

import jax
import jax.numpy as jnp
from jax import lax
from jax.experimental import pallas as pl
from jax.experimental.pallas import tpu as pltpu
from jax.sharding import PartitionSpec as P


BF16 = jnp.bfloat16
F32 = jnp.float32
VMEM = pl.BlockSpec(memory_space=pltpu.VMEM)
HBM = pl.BlockSpec(memory_space=pltpu.HBM)
MIB = 1 << 20


def factors(n):
    core = min(2, n)
    outer = min(4, n // core)
    return outer, n // core // outer, core


def zstep(k, middle, core):
    return k * middle * core + core - 1


def swap(x, n, k):
    return lax.ppermute(x, "lat", [(i, i ^ k) for i in range(n)])


def call(kernel, outs, args, specs=None, scratch=(), flops=1000000):
    return pl.pallas_call(
        kernel,
        out_shape=outs,
        in_specs=specs or [VMEM] * len(args),
        out_specs=[VMEM] * len(outs),
        scratch_shapes=list(scratch),
        compiler_params=pltpu.CompilerParams(vmem_limit_bytes=8 * MIB),
        cost_estimate=pl.CostEstimate(flops=flops, bytes_accessed=MIB, transcendentals=0),
    )(*args)


def load_kernel(count, ds, layers, *refs):
    sems = refs[2 * count]
    pairs = [(refs[i], refs[count + i]) for i in range(count)]
    if ds:
        source, dest = pairs.pop()
        layer = lax.axis_index("layer")
        pairs += [(source.at[0, lax.rem(layer + d, layers)], dest.at[0, j]) for j, d in enumerate(ds)]
    copies = [pltpu.make_async_copy(source, dest, sems.at[i]) for i, (source, dest) in enumerate(pairs)]
    for copy in copies:
        copy.start()
    for copy in copies:
        copy.wait()


def load(arrays, ds=(), layers=1):
    arrays = [pltpu.with_memory_space_constraint(a, pltpu.HBM) for a in arrays]
    shapes = [a.shape for a in arrays]
    if ds:
        shapes[-1] = (1, len(ds)) + shapes[-1][2:]
    count = len(arrays)
    return call(
        functools.partial(load_kernel, count, tuple(ds), layers),
        [jax.ShapeDtypeStruct(shape, a.dtype) for shape, a in zip(shapes, arrays)],
        arrays,
        specs=[HBM] * count,
        scratch=[pltpu.SemaphoreType.DMA((count + len(ds),))],
    )


def stack_kernel(*refs):
    out = refs[-1]
    at = 0
    for ref in refs[:-1]:
        out[pl.ds(at, ref.shape[0]), :] = ref[...]
        at += ref.shape[0]


def stack(pieces):
    rows = sum(p.shape[0] for p in pieces)
    shape = jax.ShapeDtypeStruct((rows, pieces[0].shape[1]), pieces[0].dtype)
    return call(stack_kernel, [shape], pieces)[0]


def encode(x, w_refs, b_refs, latent):
    for c, (w, b) in enumerate(zip(w_refs, b_refs)):
        size = w.shape[2]
        pre = jnp.dot(x[...], w[0], preferred_element_type=F32) + b[...]
        latent[:, c * size : (c + 1) * size] = jnp.maximum(pre, 0.0).astype(BF16)


def decode(latent, w_refs, d, layers, outs):
    target = lax.axis_index("layer") + d

    @pl.when(target < layers)
    def _():
        total = None
        for c, w in enumerate(w_refs):
            size = w.shape[2]
            part = jnp.dot(
                latent[:, c * size : (c + 1) * size],
                w[0, target if c else max(d - 1, 0)],
                preferred_element_type=F32,
            )
            total = part if total is None else total + part
        at = 0
        for out in outs:
            out[...] = total[at : at + out.shape[0]].astype(out.dtype)
            at += out.shape[0]

    if d:

        @pl.when(target >= layers)
        def _():
            for out in outs:
                out[...] = jnp.zeros_like(out)


def encode_kernel(core, slots, plan, layers, *refs):
    xs = 1 + max(at[0] for at in slots)
    x_refs, refs = refs[:xs], refs[xs:]
    w_refs, b_refs, d_refs = refs[:core], refs[core : 2 * core], refs[2 * core : 3 * core]
    latent, outs, x = refs[3 * core], refs[3 * core + 1 : -1], refs[-1]
    at = 0
    for which, first, rows in slots:
        x[pl.ds(at, rows), :] = x_refs[which][pl.ds(first, rows), :]
        at += rows
    encode(x, w_refs, b_refs, latent)
    for d, groups in plan:
        decode(latent, d_refs, d, layers, outs[:groups])
        outs = outs[groups:]


def decode_kernel(core, layers, latent, *refs):
    decode(latent, refs[:core], 0, layers, refs[core:])


def sum_kernel(ats, block, *refs):
    parts, outs = refs[: len(ats)], refs[len(ats) :]
    for j, out in enumerate(outs):
        total = None
        for at, ref in zip(ats, parts):
            part = ref[pl.ds(at + j * block, block), :].astype(F32)
            total = part if total is None else total + part
        out[...] = total.astype(out.dtype)


def work(acts, enc_weight, enc_bias, dec_weight, dec_bias):
    layers = lax.axis_size("layer")
    n = lax.axis_size("lat")
    outer, middle, core = factors(n)
    width = acts.shape[2]
    size = enc_weight.shape[2]

    pieces = [swap(acts[0], n, zstep(k, middle, core)) for k in range(1, outer)]
    enc = [swap(enc_weight, n, k) for k in range(1, core)]
    dec = [swap(dec_weight, n, k) for k in range(1, core)]
    bias = [swap(enc_bias, n, k) for k in range(1, core)]
    later = list(range(layers - 1, 0, -1))
    ahead = later[::-1]
    own, own_enc, own_bias, *own_next = load(
        [acts[0], enc_weight, enc_bias] + ([dec_weight] if ahead else []), ahead, layers
    )
    own_dec = load([dec_weight], [0], layers)[0]
    dec_next = (own_next or [own_dec]) + dec
    enc, dec, bias = [own_enc] + enc, [own_dec] + dec, [own_bias] + bias
    block = own.shape[0]
    rows = block * outer
    flops = 2 * rows * core * size * width
    hidden = jax.ShapeDtypeStruct((rows, core * size), BF16)

    blocks = [own] + pieces
    batches = [[0] + list(range(outer - 1, 0, -1))[:1], list(range(1, outer - 1))]
    batches = [batch for batch in batches if batch]
    stacks = [stack([blocks[k] for k in batch]) for batch in batches]
    slots = [None] * outer
    for i, batch in enumerate(batches):
        for j, k in enumerate(batch):
            slots[k] = (i, j * block, block)
    xs = [(blocks, [(k, 0, block) for k in range(outer)])]
    for k in range(1, middle):
        xs.append(([swap(x, n, k * core) for x in stacks], slots))

    groups = cuts(outer)
    order = [k for group in groups for k in group]

    def send(part, d, k):
        pairs = [
            (l * n + i, (l + d) % layers * n + (i ^ (k * core) if l + d < layers else i))
            for l in range(layers)
            for i in range(n)
        ]
        return lax.ppermute(part, ("layer", "lat"), pairs)

    def shapes(dtype, whole=False):
        sizes = [rows] if whole else [block * len(group) for group in groups]
        return [jax.ShapeDtypeStruct((size, width), dtype) for size in sizes]

    totals = [[] for _ in groups]
    for k, (x, where) in enumerate(xs):
        plan = [(d, len(groups) if k else 1) for d in later]
        outs = [shape for d, _ in plan for shape in shapes(BF16 if d else F32, d > 0 and k == 0)]
        latent, *parts = call(
            functools.partial(encode_kernel, core, [where[j] for j in order], plan, layers),
            [hidden] + outs,
            x + enc + bias + dec_next,
            scratch=[pltpu.VMEM((rows, width), BF16)],
            flops=flops * (1 + len(plan)),
        )
        if k == 0:
            for d in later:
                got = send(parts.pop(0), d, k)
                at = 0
                for total, group in zip(totals, groups):
                    total.append((at, got))
                    at += block * len(group)
            kept = call(
                functools.partial(decode_kernel, core, layers),
                shapes(F32),
                [latent] + dec,
                flops=flops,
            )
            for total, part in zip(totals, kept):
                total.insert(0, (0, part))
        else:
            own_parts = call(
                functools.partial(decode_kernel, core, layers),
                shapes(BF16),
                [latent] + dec,
                flops=flops,
            )
            for g, total in enumerate(totals):
                for i, d in enumerate(later):
                    total.append((0, send(parts[i * len(groups) + g], d, k)))
                total.append((0, send(own_parts[g], 0, k)))
    result = None
    near = []
    for total, group in zip(totals, groups):
        pieces = call(
            functools.partial(sum_kernel, [at for at, _ in total], block),
            [jax.ShapeDtypeStruct((block, width), BF16 if k else F32) for k in group],
            [part for _, part in total],
        )
        for k, piece in zip(group, pieces):
            if k:
                near.append(swap(piece, n, zstep(k, middle, core)))
            else:
                result = piece
    for piece in near:
        result = result + piece.astype(F32)
    return (result + dec_bias[0][None, :]).astype(BF16)[None]


def cuts(outer):
    far = list(range(outer - 1, 0, -1))
    half = len(far) - max(outer // 2 - 1, 0)
    return [group for group in (far[:half], far[half:] + [0]) if group]


def solution(mesh):
    return jax.shard_map(
        work,
        mesh=mesh,
        in_specs=(
            P("layer", "lat", None),
            P("layer", None, "lat"),
            P("layer", "lat"),
            P("layer", None, "lat", None),
            P("layer", None),
        ),
        out_specs=P("layer", "lat", None),
        check_vma=False,
    )
```
